32 devices in a mesh: prompt: 4 (over x, core), dp: 4 (over z), mp: 2 (over y).
Axes of the slice: x: 2, y: 2, z: 4, core: 2. Of those that a mesh axis runs over, the one named last changes fastest.
Arguments:
- prompts: bfloat16 [8, 100, 4096], P('prompt'), may hold values from -6 to 6
- target_embed: bfloat16 [4, 512, 4096], P('dp'), may hold values from -6 to 6
- labels: int32 [4, 512], P('dp'), may hold values from 0 to 16383
- lengths: int32 [4], P('dp'), may hold values from 128 to 512
- attn_gain: float32 [4096], replicated, may hold values from 0.5 to 1.5
- w_qkv: bfloat16 [3, 4096, 2048], P(None, None, 'mp'), may hold values from -4 to 4
- w_out: bfloat16 [2048, 4096], P('mp'), may hold values from -0.5 to 0.5
- final_gain: float32 [4096], replicated, may hold values from 0.5 to 1.5
- w_vocab: bfloat16 [4096, 16384], P(None, ('dp', 'mp')), may hold values from -3 to 3
Outputs:
- token_loss: float32 [8, 4, 512], P('prompt', 'dp')
- prompt_loss: float32 [8], replicated
The draws below stay inside these ranges and needn't reach their ends.
Inputs may be any that keep to these rules, and one draw needn't show every extreme that they name: `lengths`: positions from a sequence's length on are padding.
All inputs are finite; a program needn't handle non-finite values.
Results may differ from the reference program's by a relative error of at most 0.006.
Values may be sent and summed in bfloat16 or wider, within the bound.
A program may use at most 192 MiB of HBM per device.

```python
import math
import jax
import jax.numpy as jnp
from jax import lax

D = 4096
HEADS = 16
HD = 128
V = 16384
LP = 100
S = 512
P_SIZE = 8
B = 4
N_MP = 2


def draw_w_qkv(key, part):
    noise = jnp.clip(jax.random.normal(key, (3, D, HEADS * HD), jnp.float32), -6.0, 6.0) / math.sqrt(D)
    return jnp.clip(noise, -4.0, 4.0).astype(jnp.bfloat16)


def draw_w_vocab(key, part):
    noise = jnp.clip(jax.random.normal(key, (D, V), jnp.float32), -6.0, 6.0)
    return (noise * 0.0625).astype(jnp.bfloat16)


def with_ends(drawn, own_key, low, top_value):
    spot = [jax.random.randint(jax.random.fold_in(own_key, axis), (), 0, length) for axis, length in enumerate(drawn.shape)]
    widest = drawn.shape.index(max(drawn.shape))
    neighbour = spot[:widest] + [(spot[widest] + 1) % drawn.shape[widest]] + spot[widest + 1:]
    return drawn.at[tuple(spot)].set(low).at[tuple(neighbour)].set(top_value)


def levels(stream_key, extent, cuts, smallest, top_value):
    loudness = 1.0
    for position, parts in cuts:
        heights = jax.random.uniform(jax.random.fold_in(jax.random.fold_in(stream_key, 6), position), (parts,), jnp.float32, smallest / len(cuts), top_value / len(cuts))
        loudness = loudness * jnp.repeat(jnp.exp(heights), extent[position] // parts).reshape((-1,) + (1,) * (len(extent) - 1 - position))
    return loudness


def bell_draw(key, extent, width, bound, split=(), kind=jnp.bfloat16):
    level = levels(key, extent, split, -0.22, 0.18) if split else 1.0
    result = jax.random.normal(key, extent, jnp.float32) * width * level
    return jnp.minimum(jnp.maximum(result, -bound), bound).astype(kind)


def setup_inputs(seed: int = 0) -> dict:
    keys = jax.random.split(jax.random.key(seed), 10)
    prompts = bell_draw(keys[0], (P_SIZE, LP, D), 1.0, 6.0, ((0, 4),))
    target_embed = bell_draw(keys[1], (B, S, D), 1.0, 6.0, ((0, 4),))
    labels = with_ends(jax.random.randint(keys[2], (B, S), 0, V), jax.random.fold_in(keys[2], 1), 0, V - 1).astype(jnp.int32)
    lengths = with_ends(jax.random.randint(keys[3], (B,), S // 4, S + 1), jax.random.fold_in(keys[3], 1), S // 4, S).astype(jnp.int32)
    attn_gain = jnp.clip(1.0 + 0.1 * jax.random.normal(keys[4], (D,), jnp.float32), 0.5, 1.5)
    w_qkv = draw_w_qkv(jax.random.fold_in(keys[9], 71), 0)
    w_out = bell_draw(keys[6], (HEADS * HD, D), (HEADS * HD // 16) ** -0.5, 0.5, ((0, 2),))
    final_gain = jnp.clip(1.0 + 0.1 * jax.random.normal(keys[7], (D,), jnp.float32), 0.5, 1.5)
    w_vocab = draw_w_vocab(jax.random.fold_in(keys[9], 71), 0)
    return {"prompts": prompts, "target_embed": target_embed, "labels": labels, "lengths": lengths, "attn_gain": attn_gain, "w_qkv": w_qkv, "w_out": w_out, "final_gain": final_gain, "w_vocab": w_vocab}


EPSILON = 1e-05
BASE_THETA = 10000.0

def rms_scaled(values, gain_vec):
    widened = values.astype(jnp.float32)
    return widened * lax.rsqrt(lax.optimization_barrier(jnp.mean(widened * widened, axis=-1, keepdims=True)) + EPSILON) * gain_vec

def rotate(values, offset, head_dim):
    number_rows = values.shape[-2]
    full_width = values.shape[-1]
    per_head = values.reshape(values.shape[:-1] + (full_width // head_dim, head_dim))
    half_dim = head_dim // 2
    positions = (offset + jnp.arange(number_rows, dtype=jnp.int32)).astype(jnp.float32)
    indices_f = jnp.arange(half_dim, dtype=jnp.int32).astype(jnp.float32)
    frequency = jnp.exp(indices_f * (-2.0 * math.log(BASE_THETA) / head_dim))
    angles = positions[:, None] * frequency[None, :]
    cosine = jnp.cos(angles)[:, None, :]
    sine_part = jnp.sin(angles)[:, None, :]
    first_half = per_head[..., :half_dim]
    second_half = per_head[..., half_dim:]
    turned = jnp.concatenate([first_half * cosine - second_half * sine_part, second_half * cosine + first_half * sine_part], axis=-1)
    return turned.reshape(values.shape)

def attend(prompt_keys, prompt_vals, target_q, target_k, target_v):
    seq_count = target_q.shape[0]
    target_len = target_q.shape[1]
    prompt_len = prompt_keys.shape[0]
    heads_here = target_q.shape[2] // HD
    keys_all = jnp.concatenate([jnp.broadcast_to(prompt_keys[None], (seq_count,) + prompt_keys.shape), target_k], axis=1)
    vals_all = jnp.concatenate([jnp.broadcast_to(prompt_vals[None], (seq_count,) + prompt_vals.shape), target_v], axis=1)
    query_h = target_q.reshape(seq_count, target_len, heads_here, HD).astype(jnp.float32)
    key_h = keys_all.reshape(seq_count, prompt_len + target_len, heads_here, HD).astype(jnp.float32)
    val_h = vals_all.reshape(seq_count, prompt_len + target_len, heads_here, HD).astype(jnp.float32)
    scores = jnp.einsum('bqhe,bkhe->bhqk', query_h, key_h) * HD ** (-0.5)
    key_index = jnp.arange(prompt_len + target_len, dtype=jnp.int32)
    query_pos = prompt_len + jnp.arange(target_len, dtype=jnp.int32)
    allowed = key_index[None, :] <= query_pos[:, None]
    scores = jnp.where(allowed[None, None], scores, -1e+30)
    top_val = lax.optimization_barrier(jnp.max(scores, axis=-1, keepdims=True))
    expo = jnp.exp(scores - top_val)
    probs = (expo / lax.optimization_barrier(jnp.sum(expo, axis=-1, keepdims=True))).astype(jnp.bfloat16)
    context = jnp.einsum('bhqk,bkhe->bqhe', probs.astype(jnp.float32), val_h)
    return context.astype(jnp.bfloat16).reshape(seq_count, target_len, heads_here * HD)

def reference(prompts, target_embed, labels, lengths, attn_gain, w_qkv, w_out, final_gain, w_vocab):
    seq_count = target_embed.shape[0]
    full_width = w_qkv.shape[2]
    group_width = full_width // N_MP
    normed_target = rms_scaled(target_embed, attn_gain).astype(jnp.bfloat16)
    flat_target = normed_target.reshape(-1, D)

    def linear(rows_in, index_w):
        return jnp.dot(rows_in, w_qkv[index_w], preferred_element_type=jnp.float32).reshape(seq_count, S, full_width)
    target_q = rotate(linear(flat_target, 0), LP, HD).astype(jnp.bfloat16)
    target_k = rotate(linear(flat_target, 1), LP, HD).astype(jnp.bfloat16)
    target_v = linear(flat_target, 2).astype(jnp.bfloat16)
    normed_prompts = rms_scaled(prompts, attn_gain).astype(jnp.bfloat16)
    residual = target_embed.reshape(-1, D).astype(jnp.float32)
    valid = jnp.arange(S, dtype=jnp.int32)[None, :] < lengths[:, None]
    flat_labels = labels.reshape(-1, 1)

    def one_prompt(prompt_rows):
        prompt_k = rotate(jnp.dot(prompt_rows, w_qkv[1], preferred_element_type=jnp.float32), 0, HD).astype(jnp.bfloat16)
        prompt_v = jnp.dot(prompt_rows, w_qkv[2], preferred_element_type=jnp.float32).astype(jnp.bfloat16)
        context = attend(prompt_k, prompt_v, target_q, target_k, target_v)
        ctx_flat = context.reshape(-1, full_width)
        hidden = residual
        for group in range(N_MP):
            part = jnp.dot(ctx_flat[:, group * group_width:(group + 1) * group_width], w_out[group * group_width:(group + 1) * group_width], preferred_element_type=jnp.float32).astype(jnp.bfloat16)
            part = lax.optimization_barrier(part)
            hidden = hidden + part.astype(jnp.float32)
        normed_out = rms_scaled(hidden, final_gain).astype(jnp.bfloat16)
        logits = jnp.dot(normed_out, w_vocab, preferred_element_type=jnp.float32)
        top_val = lax.optimization_barrier(jnp.max(logits, axis=1))
        log_total = top_val + jnp.log(lax.optimization_barrier(jnp.sum(jnp.exp(logits - top_val[:, None]), axis=1)))
        picked = jnp.take_along_axis(logits, flat_labels, axis=1)[:, 0]
        losses = (log_total - picked).reshape(seq_count, S)
        return jnp.where(valid, losses, 0.0)
    token_loss = lax.map(one_prompt, normed_prompts)
    prompt_loss = lax.optimization_barrier(jnp.sum(token_loss, axis=(1, 2))) / jnp.sum(lengths).astype(jnp.float32)
    return (token_loss, prompt_loss)
```

```python
import functools
import math

import jax
import jax.numpy as jnp
from jax import lax
from jax.experimental import pallas as pl
from jax.experimental.pallas import tpu as pltpu
from jax.sharding import PartitionSpec as P


HD = 128
EPSILON = 1e-05
BASE_THETA = 10000.0
LANES = 128
NEG = -1e30


def shift_by(value, axis, hop):
    size = lax.axis_size(axis)
    return lax.ppermute(value, axis, [(i, (i + hop) % size) for i in range(size)])


def ring_source(axis, hop):
    size = lax.axis_size(axis)
    return lax.rem(lax.axis_index(axis) + size - hop, size)


def in_order(parts, axis):
    size = len(parts)
    stacked = jnp.stack(parts)
    owners = lax.axis_index(axis) + size - jnp.arange(size, dtype=jnp.int32)
    return jnp.take(stacked, lax.rem(owners, size), axis=0)


def small_gather(value, axis):
    size = lax.axis_size(axis)
    return in_order([value] + [shift_by(value, axis, k) for k in range(1, size)], axis)


def spread(piece, axis):
    size = lax.axis_size(axis)
    me = lax.axis_index(axis)
    if size & (size - 1):
        return [(piece, me)] + [(shift_by(piece, axis, k), ring_source(axis, k)) for k in range(1, size)]
    held = [(piece, me)]
    bit = size // 2
    while bit:
        pairs = [(i, i ^ bit) for i in range(size)]
        held = held + [
            (lax.ppermute(part, axis, pairs), jnp.bitwise_xor(owner, bit)) for part, owner in held
        ]
        bit //= 2
    return held


def assemble(held):
    height = held[0][0].shape[0]
    whole = jnp.zeros((len(held) * height,) + held[0][0].shape[1:], held[0][0].dtype)
    for part, owner in held:
        whole = lax.dynamic_update_slice_in_dim(whole, part, owner * height, 0)
    return whole


def peer_piece(array, axis):
    height = array.shape[0] // lax.axis_size(axis)
    return lax.dynamic_slice_in_dim(array, lax.axis_index(axis) * height, height, 0)


def rope_tables(positions):
    half = HD // 2
    frequency = jnp.exp(
        jnp.arange(half, dtype=jnp.int32).astype(jnp.float32) * (-2.0 * math.log(BASE_THETA) / HD)
    )
    angles = positions.astype(jnp.float32)[:, None] * frequency[None, :]
    cosine, sine = jnp.cos(angles), jnp.sin(angles)
    return jnp.concatenate([cosine, cosine], 1), jnp.concatenate([-sine, sine], 1)


def largest_tile(width, most):
    tile = min(width, most)
    while width % tile:
        tile -= LANES
    return tile


def qkv_body(rows_target, target_ref, prompt_ref, gain_ref, w_ref, cos_ref, sin_ref, out_ref, normed):
    which = pl.program_id(0)

    @pl.when((which == 0) & (pl.program_id(1) == 0))
    def _():
        for ref, start in ((target_ref, 0), (prompt_ref, rows_target)):
            step = 64

            def one(i, carry, ref=ref, start=start):
                lo = pl.multiple_of(i * step, step)
                wide = ref[pl.ds(lo, step), :].astype(jnp.float32)
                scale = lax.rsqrt(jnp.mean(wide * wide, axis=-1, keepdims=True) + EPSILON)
                normed[pl.ds(pl.multiple_of(start + lo, step), step), :] = (
                    wide * scale * gain_ref[...]
                ).astype(jnp.bfloat16)
                return carry

            lax.fori_loop(0, ref.shape[0] // step, one, 0)

    total = normed.shape[0]
    block = 256

    def rows(lo, turn):
        acc = jnp.dot(
            normed[lo : lo + block, :], w_ref[0], preferred_element_type=jnp.float32
        )
        for h in range(acc.shape[1] // HD):
            part = acc[:, h * HD : (h + 1) * HD]
            if turn:
                part = part * cos_ref[lo : lo + block, :] + pltpu.roll(part, HD // 2, 1) * sin_ref[lo : lo + block, :]
            out_ref[0, lo : lo + block, h * HD : (h + 1) * HD] = part.astype(jnp.bfloat16)

    @pl.when(which == 0)
    def _():
        for lo in range(0, rows_target, block):
            rows(lo, True)
        out_ref[0, rows_target:, :] = jnp.zeros((total - rows_target, out_ref.shape[2]), jnp.bfloat16)

    @pl.when(which == 1)
    def _():
        for lo in range(0, total, block):
            rows(lo, True)

    @pl.when(which == 2)
    def _():
        for lo in range(0, total, block):
            rows(lo, False)


def project(target_rows, prompt_rows, gain, w_qkv, cosine, sine):
    rows_target, depth = target_rows.shape
    total = rows_target + prompt_rows.shape[0]
    width = w_qkv.shape[2]
    tile = largest_tile(width, 512)
    return pl.pallas_call(
        functools.partial(qkv_body, rows_target),
        grid=(3, width // tile),
        in_specs=[
            pl.BlockSpec((rows_target, depth), lambda c, j: (0, 0)),
            pl.BlockSpec(prompt_rows.shape, lambda c, j: (0, 0)),
            pl.BlockSpec((1, depth), lambda c, j: (0, 0)),
            pl.BlockSpec((1, depth, tile), lambda c, j: (c, 0, j)),
            pl.BlockSpec((total, HD), lambda c, j: (0, 0)),
            pl.BlockSpec((total, HD), lambda c, j: (0, 0)),
        ],
        out_specs=pl.BlockSpec((1, total, tile), lambda c, j: (c, 0, j)),
        out_shape=jax.ShapeDtypeStruct((3, total, width), jnp.bfloat16),
        scratch_shapes=[pltpu.VMEM((total, depth), jnp.bfloat16)],
        cost_estimate=pl.CostEstimate(
            flops=6 * total * depth * width, bytes_accessed=6 * depth * width, transcendentals=0
        ),
        name="qkv_rope",
    )(target_rows, prompt_rows, gain.reshape(1, -1), w_qkv, cosine, sine)


def attend_body(prompts_here, target_len, seqs, prompt_len, pad_len, q_ref, k_ref, v_ref, out_ref):
    scale = HD ** (-0.5)
    block = 256 if target_len % 256 == 0 else target_len
    rows_target = seqs * target_len
    contract = (((1,), (1,)), ((), ()))
    col = lax.broadcasted_iota(jnp.int32, (block, pad_len), 1)
    for b in range(seqs):
        base = b * target_len
        for i in range(target_len // block):
            lo = base + i * block
            reach = (i + 1) * block
            query = q_ref[0, lo : lo + block, :]
            s = lax.dot_general(
                query, k_ref[0, base : base + reach, :], contract, preferred_element_type=jnp.float32
            ) * scale
            row_id = lax.broadcasted_iota(jnp.int32, s.shape, 0) + i * block
            col_id = lax.broadcasted_iota(jnp.int32, s.shape, 1)
            s = jnp.where(col_id <= row_id, s, NEG)
            top = jnp.max(s, axis=1, keepdims=True)
            p = jnp.exp(s - top)
            mass = jnp.sum(p, axis=1, keepdims=True)
            own = jnp.dot(
                p.astype(jnp.bfloat16), v_ref[0, base : base + reach, :], preferred_element_type=jnp.float32
            )
            for j in range(prompts_here):
                at = rows_target + j * pad_len
                s1 = lax.dot_general(
                    query, k_ref[0, at : at + pad_len, :], contract, preferred_element_type=jnp.float32
                ) * scale
                s1 = jnp.where(col < prompt_len, s1, NEG)
                peak = jnp.maximum(top, jnp.max(s1, axis=1, keepdims=True))
                p1 = jnp.exp(s1 - peak)
                keep = jnp.exp(top - peak)
                whole = mass * keep + jnp.sum(p1, axis=1, keepdims=True)
                got = own * keep + jnp.dot(
                    p1.astype(jnp.bfloat16), v_ref[0, at : at + pad_len, :], preferred_element_type=jnp.float32
                )
                out_ref[j, lo : lo + block, :] = (got / whole).astype(jnp.bfloat16)


def attend(qkv, prompts_here, target_len, seqs, prompt_len, pad_len):
    total, width = qkv.shape[1:]
    heads = width // HD
    rows_target = seqs * target_len
    return pl.pallas_call(
        functools.partial(attend_body, prompts_here, target_len, seqs, prompt_len, pad_len),
        grid=(heads,),
        in_specs=[
            pl.BlockSpec((1, total, HD), lambda h, c=c: (c, 0, h)) for c in range(3)
        ],
        out_specs=pl.BlockSpec((prompts_here, rows_target, HD), lambda h: (0, 0, h)),
        out_shape=jax.ShapeDtypeStruct((prompts_here, rows_target, width), jnp.bfloat16),
        cost_estimate=pl.CostEstimate(
            flops=10 * heads * rows_target * target_len * HD, bytes_accessed=8 * total * width, transcendentals=0
        ),
        name="attend",
    )(qkv, qkv, qkv)


def out_body(piece_count, owners_ref, ctx_ref, other_ref, embed_ref, gain_ref, w_ref, *rest):
    piece_refs = rest[:piece_count]
    out_ref, hidden, squares, turned = rest[piece_count:]
    j = pl.program_id(0)
    tile = w_ref.shape[1]
    rows = ctx_ref.shape[0]

    @pl.when(j == 0)
    def _():
        low = 0
        for n, ref in enumerate(piece_refs):
            high = ref.shape[0]
            at = pl.multiple_of(owners_ref[n], 128)
            turned[:, low : low + high] = other_ref[:, pl.ds(at, high)]
            low += high
        squares[...] = jnp.zeros(squares.shape, jnp.float32)

    weights = jnp.concatenate([ref[...] for ref in piece_refs], axis=0)
    block = 256 if rows % 256 == 0 else rows
    for lo in range(0, rows, block):
        acc = jnp.dot(ctx_ref[lo : lo + block, :], w_ref[...], preferred_element_type=jnp.float32)
        acc += jnp.dot(turned[lo : lo + block, :], weights, preferred_element_type=jnp.float32)
        acc += embed_ref[lo : lo + block, :].astype(jnp.float32)
        hidden[j, lo : lo + block, :] = acc
        part = acc[:, :LANES] * acc[:, :LANES]
        for g in range(LANES, tile, LANES):
            part += acc[:, g : g + LANES] * acc[:, g : g + LANES]
        squares[lo : lo + block, :] += part

    @pl.when(j == pl.num_programs(0) - 1)
    def _():
        steps = hidden.shape[0]
        mean = jnp.sum(squares[...], axis=1, keepdims=True) / (steps * tile)
        scale = lax.rsqrt(mean + EPSILON)
        for n in range(steps):
            out_ref[:, n * tile : (n + 1) * tile] = (
                hidden[n] * scale * gain_ref[:, n * tile : (n + 1) * tile]
            ).astype(jnp.bfloat16)


def out_project(ctx, other, embed, gain, w_own, pieces, offsets):
    total, depth = ctx.shape
    width = w_own.shape[1]
    tile = largest_tile(width, 512)
    rows = total
    line = lambda j, *_: (0, 0)
    column = lambda j, *_: (0, j)
    return pl.pallas_call(
        functools.partial(out_body, len(pieces)),
        grid_spec=pltpu.PrefetchScalarGridSpec(
            num_scalar_prefetch=1,
            grid=(width // tile,),
            in_specs=[
                pl.BlockSpec((rows, depth), line),
                pl.BlockSpec((rows, other.shape[1]), line),
                pl.BlockSpec((rows, tile), lambda j, *_: (0, j)),
                pl.BlockSpec((1, width), lambda j, *_: (0, 0)),
                pl.BlockSpec((w_own.shape[0], tile), column),
            ]
            + [pl.BlockSpec((piece.shape[0], tile), column) for piece in pieces],
            out_specs=pl.BlockSpec((rows, width), line),
            scratch_shapes=[
                pltpu.VMEM((width // tile, rows, tile), jnp.float32),
                pltpu.VMEM((rows, LANES), jnp.float32),
                pltpu.VMEM((rows, other.shape[1]), jnp.bfloat16),
            ],
        ),
        out_shape=jax.ShapeDtypeStruct((total, width), jnp.bfloat16),
        cost_estimate=pl.CostEstimate(
            flops=2 * total * (depth + other.shape[1]) * width, bytes_accessed=4 * depth * width, transcendentals=0
        ),
        name="out_project",
    )(offsets, ctx, other, embed, gain.reshape(1, -1), w_own, *pieces)


def vocab_body(piece_count, scalars_ref, rows_ref, labels_ref, top_in, mass_in, pick_in, *rest):
    piece_refs = rest[:piece_count]
    top_ref, mass_ref, pick_ref = rest[piece_count:]
    j = pl.program_id(0)
    tile = piece_refs[0].shape[1]
    rows = rows_ref.shape[0]

    @pl.when(j == 0)
    def _():
        top_ref[...] = top_in[...]
        mass_ref[...] = mass_in[...]
        pick_ref[...] = pick_in[...]

    first = scalars_ref[0] + j * tile
    block = 256 if rows % 256 == 0 else rows
    for lo in range(0, rows, block):
        acc = None
        for n, ref in enumerate(piece_refs):
            high = ref.shape[0]
            if piece_count == 1:
                left = rows_ref[lo : lo + block, :]
            else:
                at = pl.multiple_of(scalars_ref[1 + n], 128)
                left = rows_ref[lo : lo + block, pl.ds(at, high)]
            part = jnp.dot(left, ref[...], preferred_element_type=jnp.float32)
            acc = part if acc is None else acc + part
        wanted = labels_ref[lo : lo + block, :] - first
        lane = lax.broadcasted_iota(jnp.int32, (block, LANES), 1)
        groups = [acc[:, g : g + LANES] for g in range(0, tile, LANES)]
        before = top_ref[lo : lo + block, :]
        now = before
        for g in groups:
            now = jnp.maximum(now, g)
        mass = mass_ref[lo : lo + block, :] * jnp.exp(before - now)
        pick = pick_ref[lo : lo + block, :]
        for n, g in enumerate(groups):
            mass += jnp.exp(g - now)
            pick += jnp.where(lane == wanted - n * LANES, g, 0.0)
        top_ref[lo : lo + block, :] = now
        mass_ref[lo : lo + block, :] = mass
        pick_ref[lo : lo + block, :] = pick


def vocab_stats(normed, labels, pieces, scalars, stats):
    rows, depth = normed.shape
    width = pieces[0].shape[1]
    tile = largest_tile(width, 512)
    fixed = lambda j, *_: (0, 0)
    lanes = pl.BlockSpec((rows, LANES), fixed)
    return pl.pallas_call(
        functools.partial(vocab_body, len(pieces)),
        grid_spec=pltpu.PrefetchScalarGridSpec(
            num_scalar_prefetch=1,
            grid=(width // tile,),
            in_specs=[pl.BlockSpec((rows, depth), fixed), pl.BlockSpec((rows, 1), fixed)]
            + [lanes] * 3
            + [pl.BlockSpec((piece.shape[0], tile), lambda j, *_: (0, j)) for piece in pieces],
            out_specs=[lanes] * 3,
        ),
        out_shape=[jax.ShapeDtypeStruct((rows, LANES), jnp.float32)] * 3,
        cost_estimate=pl.CostEstimate(
            flops=2 * rows * depth * width, bytes_accessed=2 * depth * width, transcendentals=0
        ),
        name="vocab_stats",
    )(scalars, normed, labels.reshape(-1, 1), *stats, *pieces)


def fresh_stats(rows):
    zero = jnp.zeros((rows, LANES), jnp.float32)
    return (jnp.full((rows, LANES), NEG, jnp.float32), zero, zero)


def fold_lanes(stats):
    top, mass, pick = stats
    peak = jnp.max(top, axis=1)
    return jnp.stack([peak, jnp.sum(mass * jnp.exp(top - peak[:, None]), axis=1), jnp.sum(pick, axis=1)])


def combine_stats(earlier, later):
    top_val = jnp.maximum(earlier[0], later[0])
    sum_exp = earlier[1] * jnp.exp(earlier[0] - top_val) + later[1] * jnp.exp(later[0] - top_val)
    return jnp.stack((top_val, sum_exp, earlier[2] + later[2]))


def swap_pair(value, axis):
    size = lax.axis_size(axis)
    return lax.ppermute(value, axis, [(i, i ^ 1) for i in range(size)])


def shards(prompts, target_embed, labels, lengths, attn_gain, w_qkv, w_out, final_gain, w_vocab):
    n_model = lax.axis_size("mp")
    n_seq = lax.axis_size("dp")
    my_seq = lax.axis_index("dp")
    prompts_here, prompt_len, model_width = prompts.shape
    seq_count, target_len, _ = target_embed.shape
    hops = range(1, n_model)
    paired = n_seq % 2 == 0
    stride = 2 if paired else 1
    unit = seq_count * target_len

    got_out = []
    for k in hops:
        got_out.append(shift_by(peer_piece(w_out, "prompt"), "mp", k))
    flat_embed = target_embed.reshape(-1, model_width)
    if paired:
        got_embed = swap_pair(peer_piece(flat_embed, "prompt"), "dp")
    parts = 4 if w_vocab.shape[1] % 512 == 0 else 1
    part_cols = w_vocab.shape[1] // parts
    vocab_jobs = [(k, c) for k in range(stride, n_seq, stride) for c in range(parts)]
    own_piece = peer_piece(w_vocab, "prompt")

    def fetch(n):
        k, c = vocab_jobs[n]
        return shift_by(own_piece[:, c * part_cols : (c + 1) * part_cols], "dp", k)

    got_vocab = [fetch(0)]

    pad_len = -(-prompt_len // 128) * 128
    positions = jnp.concatenate(
        [prompt_len + jnp.arange(target_len, dtype=jnp.int32)] * seq_count
        + [jnp.arange(pad_len, dtype=jnp.int32)] * prompts_here
    )
    cosine, sine = rope_tables(positions)
    padded = jnp.pad(prompts, ((0, 0), (0, pad_len - prompt_len), (0, 0))).reshape(-1, model_width)
    qkv = project(flat_embed, padded, attn_gain, w_qkv, cosine, sine)
    ctx = attend(qkv, prompts_here, target_len, seq_count, prompt_len, pad_len)
    ctx = ctx.reshape(prompts_here * unit, -1)

    if paired:
        ctx_pair = swap_pair(ctx, "dp")
    other_a = jnp.concatenate([shift_by(ctx, "mp", k) for k in hops], axis=1)
    for n in range(1, len(vocab_jobs)):
        got_vocab.append(fetch(n))

    out_pieces, out_offsets = [], []
    for n, got in enumerate(got_out):
        held = spread(got, "prompt")
        if got.shape[0] % LANES:
            held = [(assemble(held), jnp.int32(0))]
        for piece, owner in held:
            out_pieces.append(piece)
            out_offsets.append(n * w_out.shape[0] + owner * piece.shape[0])
    out_offsets = jnp.stack(out_offsets).astype(jnp.int32)

    vocab_sets = []
    for n, got in enumerate(got_vocab):
        held = spread(got, "prompt")
        first = (ring_source("dp", vocab_jobs[n][0]) * n_model + lax.axis_index("mp")) * w_vocab.shape[1]
        first = first + vocab_jobs[n][1] * part_cols
        scalars = jnp.stack([first] + [o * p.shape[0] for p, o in held]).astype(jnp.int32)
        vocab_sets.append(([p for p, _ in held], scalars))

    def tiled(flat):
        return jnp.tile(flat, (prompts_here,) + (1,) * (flat.ndim - 1))

    own_first = ((my_seq * n_model + lax.axis_index("mp")) * w_vocab.shape[1]).astype(jnp.int32)
    own_scalars = jnp.stack([own_first, jnp.int32(0)])
    sets = []
    rows = out_project(ctx, other_a, tiled(flat_embed), final_gain, w_out, out_pieces, out_offsets)
    ids = tiled(labels.reshape(-1))
    stats = vocab_stats(rows, ids, [w_vocab], own_scalars, fresh_stats(rows.shape[0]))
    sets.append([rows, ids, stats])
    if paired:
        other_b = jnp.concatenate([shift_by(ctx_pair, "mp", k) for k in hops], axis=1)
        embed_pair = assemble(spread(got_embed, "prompt"))
        ids = tiled(swap_pair(labels.reshape(-1), "dp"))
        rows = out_project(ctx_pair, other_b, tiled(embed_pair), final_gain, w_out, out_pieces, out_offsets)
        stats = vocab_stats(rows, ids, [w_vocab], own_scalars, fresh_stats(rows.shape[0]))
        sets.append([rows, ids, stats])
    for pieces, scalars in vocab_sets:
        for entry in sets:
            entry[2] = vocab_stats(entry[0], entry[1], pieces, scalars, entry[2])

    merged = fold_lanes(sets[0][2])
    if paired:
        merged = combine_stats(merged, swap_pair(fold_lanes(sets[1][2]), "dp"))
    for other in [shift_by(merged, "mp", k) for k in hops]:
        merged = combine_stats(merged, other)
    losses = merged[0] + jnp.log(merged[1]) - merged[2]
    losses = losses.reshape(prompts_here, seq_count, target_len)
    valid = jnp.arange(target_len, dtype=jnp.int32)[None, :] < lengths[:, None]
    token_loss = jnp.where(valid[None], losses, 0.0)
    prompt_sums = jnp.sum(token_loss, axis=(1, 2))
    counted = jnp.sum(lengths).astype(jnp.float32)
    sums = jnp.sum(small_gather(jnp.concatenate([prompt_sums, counted[None]]), "dp"), axis=0)
    table = small_gather(sums, "prompt")
    prompt_loss = table[:, :prompts_here].reshape(-1) / table[0, prompts_here]
    return (token_loss, prompt_loss)


def solution(mesh):
    return jax.shard_map(
        shards,
        mesh=mesh,
        in_specs=(
            P("prompt", None, None),
            P("dp", None, None),
            P("dp", None),
            P("dp"),
            P(),
            P(None, None, "mp"),
            P("mp", None),
            P(),
            P(None, ("dp", "mp")),
        ),
        out_specs=(P("prompt", "dp", None), P()),
        check_vma=False,
    )
```

```python
import functools
import math

import jax
import jax.numpy as jnp
from jax import lax
from jax.experimental import pallas as pl
from jax.experimental.pallas import tpu as pltpu
from jax.sharding import PartitionSpec as P


HD = 128
EPSILON = 1e-05
BASE_THETA = 10000.0
LANES = 128
NEG = -1e30


def shift_by(value, axis, hop):
    size = lax.axis_size(axis)
    return lax.ppermute(value, axis, [(i, (i + hop) % size) for i in range(size)])


def ring_source(axis, hop):
    size = lax.axis_size(axis)
    return lax.rem(lax.axis_index(axis) + size - hop, size)


def in_order(parts, axis):
    size = len(parts)
    stacked = jnp.stack(parts)
    owners = lax.axis_index(axis) + size - jnp.arange(size, dtype=jnp.int32)
    return jnp.take(stacked, lax.rem(owners, size), axis=0)


def small_gather(value, axis):
    size = lax.axis_size(axis)
    return in_order([value] + [shift_by(value, axis, k) for k in range(1, size)], axis)


def spread(piece, axis):
    size = lax.axis_size(axis)
    me = lax.axis_index(axis)
    if size & (size - 1):
        return [(piece, me)] + [(shift_by(piece, axis, k), ring_source(axis, k)) for k in range(1, size)]
    held = [(piece, me)]
    bit = size // 2
    while bit:
        pairs = [(i, i ^ bit) for i in range(size)]
        held = held + [
            (lax.ppermute(part, axis, pairs), jnp.bitwise_xor(owner, bit)) for part, owner in held
        ]
        bit //= 2
    return held


def assemble(held):
    height = held[0][0].shape[0]
    whole = jnp.zeros((len(held) * height,) + held[0][0].shape[1:], held[0][0].dtype)
    for part, owner in held:
        whole = lax.dynamic_update_slice_in_dim(whole, part, owner * height, 0)
    return whole


def peer_piece(array, axis):
    height = array.shape[0] // lax.axis_size(axis)
    return lax.dynamic_slice_in_dim(array, lax.axis_index(axis) * height, height, 0)


def rope_tables(positions):
    half = HD // 2
    frequency = jnp.exp(
        jnp.arange(half, dtype=jnp.int32).astype(jnp.float32) * (-2.0 * math.log(BASE_THETA) / HD)
    )
    angles = positions.astype(jnp.float32)[:, None] * frequency[None, :]
    cosine, sine = jnp.cos(angles), jnp.sin(angles)
    return jnp.concatenate([cosine, cosine], 1), jnp.concatenate([-sine, sine], 1)


def largest_tile(width, most):
    tile = min(width, most)
    while width % tile:
        tile -= LANES
    return tile


def qkv_body(rows_target, target_ref, prompt_ref, gain_ref, w_ref, cos_ref, sin_ref, out_ref, normed):
    which = pl.program_id(0)

    @pl.when((which == 0) & (pl.program_id(1) == 0))
    def _():
        def normal(raw):
            wide = raw.astype(jnp.float32)
            scale = lax.rsqrt(jnp.mean(wide * wide, axis=-1, keepdims=True) + EPSILON)
            return (wide * scale * gain_ref[...]).astype(jnp.bfloat16)

        step = 64

        def one(i, carry):
            at = pl.ds(pl.multiple_of(i * step, step), step)
            normed[at, :] = normal(target_ref[at, :])
            return carry

        lax.fori_loop(0, rows_target // step, one, 0)
        count, length, depth = prompt_ref.shape
        span = (normed.shape[0] - rows_target) // count
        for p in range(count):
            base = rows_target + p * span
            for lo in range(0, length, step):
                high = min(length, lo + step)
                normed[base + lo : base + high, :] = normal(prompt_ref[p, lo:high, :])
            if span > length:
                normed[base + length : base + span, :] = jnp.zeros((span - length, depth), jnp.bfloat16)

    total = normed.shape[0]
    block = 256

    def rows(lo, turn):
        acc = jnp.dot(
            normed[lo : lo + block, :], w_ref[0], preferred_element_type=jnp.float32
        )
        for h in range(acc.shape[1] // HD):
            part = acc[:, h * HD : (h + 1) * HD]
            if turn:
                part = part * cos_ref[lo : lo + block, :] + pltpu.roll(part, HD // 2, 1) * sin_ref[lo : lo + block, :]
            out_ref[0, lo : lo + block, h * HD : (h + 1) * HD] = part.astype(jnp.bfloat16)

    @pl.when(which == 0)
    def _():
        for lo in range(0, rows_target, block):
            rows(lo, True)
        out_ref[0, rows_target:, :] = jnp.zeros((total - rows_target, out_ref.shape[2]), jnp.bfloat16)

    @pl.when(which == 1)
    def _():
        for lo in range(0, total, block):
            rows(lo, True)

    @pl.when(which == 2)
    def _():
        for lo in range(0, total, block):
            rows(lo, False)


def project(target_rows, prompts, pad_len, gain, w_qkv, cosine, sine):
    rows_target, depth = target_rows.shape
    total = rows_target + prompts.shape[0] * pad_len
    width = w_qkv.shape[2]
    tile = largest_tile(width, 512)
    return pl.pallas_call(
        functools.partial(qkv_body, rows_target),
        grid=(3, width // tile),
        in_specs=[
            pl.BlockSpec((rows_target, depth), lambda c, j: (0, 0)),
            pl.BlockSpec(prompts.shape, lambda c, j: (0, 0, 0)),
            pl.BlockSpec((1, depth), lambda c, j: (0, 0)),
            pl.BlockSpec((1, depth, tile), lambda c, j: (c, 0, j)),
            pl.BlockSpec((total, HD), lambda c, j: (0, 0)),
            pl.BlockSpec((total, HD), lambda c, j: (0, 0)),
        ],
        out_specs=pl.BlockSpec((1, total, tile), lambda c, j: (c, 0, j)),
        out_shape=jax.ShapeDtypeStruct((3, total, width), jnp.bfloat16),
        scratch_shapes=[pltpu.VMEM((total, depth), jnp.bfloat16)],
        cost_estimate=pl.CostEstimate(
            flops=6 * total * depth * width, bytes_accessed=6 * depth * width, transcendentals=0
        ),
        name="qkv_rope",
    )(target_rows, prompts, gain.reshape(1, -1), w_qkv, cosine, sine)


def attend_body(prompts_here, target_len, seqs, prompt_len, pad_len, q_ref, k_ref, v_ref, out_ref):
    scale = HD ** (-0.5)
    block = 256 if target_len % 256 == 0 else target_len
    rows_target = seqs * target_len
    contract = (((1,), (1,)), ((), ()))
    col = lax.broadcasted_iota(jnp.int32, (block, pad_len), 1)
    for b in range(seqs):
        base = b * target_len
        for i in range(target_len // block):
            lo = base + i * block
            reach = (i + 1) * block
            query = q_ref[0, lo : lo + block, :]
            s = lax.dot_general(
                query, k_ref[0, base : base + reach, :], contract, preferred_element_type=jnp.float32
            ) * scale
            row_id = lax.broadcasted_iota(jnp.int32, s.shape, 0) + i * block
            col_id = lax.broadcasted_iota(jnp.int32, s.shape, 1)
            s = jnp.where(col_id <= row_id, s, NEG)
            top = jnp.max(s, axis=1, keepdims=True)
            p = jnp.exp(s - top)
            mass = jnp.sum(p, axis=1, keepdims=True)
            own = jnp.dot(
                p.astype(jnp.bfloat16), v_ref[0, base : base + reach, :], preferred_element_type=jnp.float32
            )
            for j in range(prompts_here):
                at = rows_target + j * pad_len
                s1 = lax.dot_general(
                    query, k_ref[0, at : at + pad_len, :], contract, preferred_element_type=jnp.float32
                ) * scale
                s1 = jnp.where(col < prompt_len, s1, NEG)
                peak = jnp.maximum(top, jnp.max(s1, axis=1, keepdims=True))
                p1 = jnp.exp(s1 - peak)
                keep = jnp.exp(top - peak)
                whole = mass * keep + jnp.sum(p1, axis=1, keepdims=True)
                got = own * keep + jnp.dot(
                    p1.astype(jnp.bfloat16), v_ref[0, at : at + pad_len, :], preferred_element_type=jnp.float32
                )
                out_ref[j, lo : lo + block, :] = (got / whole).astype(jnp.bfloat16)


def attend(qkv, prompts_here, target_len, seqs, prompt_len, pad_len):
    total, width = qkv.shape[1:]
    heads = width // HD
    rows_target = seqs * target_len
    return pl.pallas_call(
        functools.partial(attend_body, prompts_here, target_len, seqs, prompt_len, pad_len),
        grid=(heads,),
        in_specs=[
            pl.BlockSpec((1, total, HD), lambda h, c=c: (c, 0, h)) for c in range(3)
        ],
        out_specs=pl.BlockSpec((prompts_here, rows_target, HD), lambda h: (0, 0, h)),
        out_shape=jax.ShapeDtypeStruct((prompts_here, rows_target, width), jnp.bfloat16),
        cost_estimate=pl.CostEstimate(
            flops=10 * heads * rows_target * target_len * HD, bytes_accessed=8 * total * width, transcendentals=0
        ),
        name="attend",
    )(qkv, qkv, qkv)


def gather_logits(acc, first, labels, before, mass, pick):
    wanted = labels - first
    lane = lax.broadcasted_iota(jnp.int32, before.shape, 1)
    groups = [acc[:, g : g + LANES] for g in range(0, acc.shape[1], LANES)]
    now = before
    for g in groups:
        now = jnp.maximum(now, g)
    mass = mass * jnp.exp(before - now)
    for n, g in enumerate(groups):
        mass += jnp.exp(g - now)
        pick += jnp.where(lane == wanted - n * LANES, g, 0.0)
    return now, mass, pick


def score_body(n_out, n_embed, steps_out, carried, scalars_ref, *refs):
    ctx_ref, other_ref, gain_ref, labels_ref, w_ref, vocab_ref = refs[:6]
    piece_refs = refs[6 : 6 + n_out]
    embed_refs = refs[6 + n_out : 6 + n_out + n_embed]
    refs = refs[6 + n_out + n_embed + carried :]
    rows_ref, scale_ref, top_ref, mass_ref, pick_ref, squares, joined, weights, embed_s = refs
    j = pl.program_id(0)
    tile = w_ref.shape[1]
    rows = ctx_ref.shape[0]
    unit = embed_s.shape[0]
    block = 256 if unit % 256 == 0 else unit

    @pl.when(j == 0)
    def _():
        joined[:, : ctx_ref.shape[1]] = ctx_ref[...]
        joined[:, ctx_ref.shape[1] :] = other_ref[...]
        squares[...] = jnp.zeros(squares.shape, jnp.float32)
        top_ref[0] = jnp.full(top_ref.shape[1:], NEG, jnp.float32)
        mass_ref[0] = jnp.zeros(mass_ref.shape[1:], jnp.float32)
        pick_ref[0] = jnp.zeros(pick_ref.shape[1:], jnp.float32)

    @pl.when(j < steps_out)
    def _():
        for n, ref in enumerate(embed_refs):
            high = ref.shape[0]
            at = pl.multiple_of(scalars_ref[1 + n_out + n], math.gcd(high, 128))
            embed_s[pl.ds(at, high), :] = ref[...]
        local = w_ref.shape[0]
        weights[:local, :] = w_ref[...]
        for n, ref in enumerate(piece_refs):
            high = ref.shape[0]
            weights[pl.ds(pl.multiple_of(local + scalars_ref[1 + n], 128), high), :] = ref[...]
        for lo in range(0, rows, block):
            acc = jnp.dot(joined[lo : lo + block, :], weights[...], preferred_element_type=jnp.float32)
            acc += embed_s[lo % unit : lo % unit + block, :].astype(jnp.float32)
            at = pl.ds(pl.multiple_of(j * tile, LANES), tile)
            rows_ref[0, lo : lo + block, at] = (acc * gain_ref[...]).astype(jnp.bfloat16)
            part = squares[lo : lo + block, :]
            for g in range(0, tile, LANES):
                part += acc[:, g : g + LANES] * acc[:, g : g + LANES]
            squares[lo : lo + block, :] = part

    @pl.when(j == steps_out - 1)
    def _():
        mean = jnp.sum(squares[...], axis=1, keepdims=True) / (steps_out * tile)
        scale_ref[0] = jnp.broadcast_to(lax.rsqrt(mean + EPSILON), squares.shape)

    @pl.when(j >= steps_out)
    def _():
        first = scalars_ref[0] + (j - steps_out) * vocab_ref.shape[1]
        for lo in range(0, rows, block):
            at = slice(lo, lo + block)
            acc = jnp.dot(rows_ref[0, at, :], vocab_ref[...], preferred_element_type=jnp.float32)
            acc = acc * scale_ref[0, at, :1]
            top_ref[0, at, :], mass_ref[0, at, :], pick_ref[0, at, :] = gather_logits(
                acc, first, labels_ref[at, :], top_ref[0, at, :], mass_ref[0, at, :], pick_ref[0, at, :]
            )


def score_own(index, count, before, ctx, other, gain, labels, w_own, w_vocab, pieces, embeds, scalars):
    rows, depth = ctx.shape
    width = w_own.shape[1]
    tile = largest_tile(width, 512)
    steps_out = width // tile
    vocab_tile = largest_tile(w_vocab.shape[1], 512)
    unit = sum(e.shape[0] for e in embeds)
    fixed = lambda j, *_: (0, 0)
    column = lambda j, *_: (0, jnp.minimum(j, steps_out - 1))
    mine = lambda j, *_: (index, 0, 0)
    shapes = [((count, rows, width), jnp.bfloat16)] + [((count, rows, LANES), jnp.float32)] * 4
    return pl.pallas_call(
        functools.partial(score_body, len(pieces), len(embeds), steps_out, len(before)),
        grid_spec=pltpu.PrefetchScalarGridSpec(
            num_scalar_prefetch=1,
            grid=(steps_out + w_vocab.shape[1] // vocab_tile,),
            in_specs=[
                pl.BlockSpec((rows, depth), fixed),
                pl.BlockSpec((rows, other.shape[1]), fixed),
                pl.BlockSpec((1, tile), column),
                pl.BlockSpec((rows, 1), fixed),
                pl.BlockSpec((w_own.shape[0], tile), column),
                pl.BlockSpec((width, vocab_tile), lambda j, *_: (0, jnp.maximum(j - steps_out, 0))),
            ]
            + [pl.BlockSpec((piece.shape[0], tile), column) for piece in pieces]
            + [pl.BlockSpec((e.shape[0], tile), column) for e in embeds]
            + [pl.BlockSpec(memory_space=pl.ANY)] * len(before),
            out_specs=[pl.BlockSpec((1, rows, width), mine)] + [pl.BlockSpec((1, rows, LANES), mine)] * 4,
            scratch_shapes=[
                pltpu.VMEM((rows, LANES), jnp.float32),
                pltpu.VMEM((rows, depth + other.shape[1]), jnp.bfloat16),
                pltpu.VMEM((depth + other.shape[1], tile), jnp.bfloat16),
                pltpu.VMEM((unit, tile), jnp.bfloat16),
            ],
        ),
        out_shape=[jax.ShapeDtypeStruct(*shape) for shape in shapes],
        input_output_aliases={7 + len(pieces) + len(embeds) + n: n for n in range(len(before))},
        cost_estimate=pl.CostEstimate(
            flops=2 * rows * width * (depth + other.shape[1] + w_vocab.shape[1]),
            bytes_accessed=2 * width * (2 * depth + w_vocab.shape[1]),
            transcendentals=0,
        ),
        name="score_own",
    )(scalars, ctx, other, gain.reshape(1, -1), labels.reshape(-1, 1), w_own, w_vocab, *pieces, *embeds, *before)


def far_body(piece_count, scalars_ref, rows_ref, scale_ref, labels_ref, top_in, mass_in, pick_in, *rest):
    piece_refs = rest[:piece_count]
    top_ref, mass_ref, pick_ref, weights = rest[piece_count:]
    rows = rows_ref.shape[0]
    block = 256 if rows % 256 == 0 else rows

    @pl.when(pl.program_id(0) == 0)
    def _():
        for n, ref in enumerate(piece_refs):
            high = ref.shape[0]
            weights[pl.ds(pl.multiple_of(scalars_ref[1 + n], 128), high), :] = ref[...]

    for lo in range(0, rows, block):
        at = slice(lo, lo + block)
        acc = jnp.dot(rows_ref[at, :], weights[...], preferred_element_type=jnp.float32)
        acc = acc * scale_ref[at, :1]
        top_ref[at, :], mass_ref[at, :], pick_ref[at, :] = gather_logits(
            acc, scalars_ref[0], labels_ref[at, :], top_in[at, :], mass_in[at, :], pick_in[at, :]
        )


def score_far(rows, scale, labels, stats, pieces, scalars):
    total, depth = rows.shape
    width = pieces[0].shape[1]
    block = math.gcd(total, 512)
    line = lambda i, *_: (i, 0)
    lanes = pl.BlockSpec((block, LANES), line)
    return pl.pallas_call(
        functools.partial(far_body, len(pieces)),
        grid_spec=pltpu.PrefetchScalarGridSpec(
            num_scalar_prefetch=1,
            grid=(total // block,),
            in_specs=[pl.BlockSpec((block, depth), line), lanes, pl.BlockSpec((block, 1), line)]
            + [lanes] * 3
            + [pl.BlockSpec(piece.shape, lambda i, *_: (0, 0)) for piece in pieces],
            out_specs=[lanes] * 3,
            scratch_shapes=[pltpu.VMEM((depth, width), jnp.bfloat16)],
        ),
        out_shape=[jax.ShapeDtypeStruct((total, LANES), jnp.float32)] * 3,
        cost_estimate=pl.CostEstimate(
            flops=2 * total * depth * width, bytes_accessed=2 * depth * (width + total), transcendentals=0
        ),
        name="score_far",
    )(scalars, rows, scale, labels.reshape(-1, 1), *stats, *pieces)


def fold_lanes(stats):
    top, mass, pick = stats
    peak = jnp.max(top, axis=1)
    return jnp.stack([peak, jnp.sum(mass * jnp.exp(top - peak[:, None]), axis=1), jnp.sum(pick, axis=1)])


def combine_stats(earlier, later):
    top_val = jnp.maximum(earlier[0], later[0])
    sum_exp = earlier[1] * jnp.exp(earlier[0] - top_val) + later[1] * jnp.exp(later[0] - top_val)
    return jnp.stack((top_val, sum_exp, earlier[2] + later[2]))


def swap_pair(value, axis):
    size = lax.axis_size(axis)
    return lax.ppermute(value, axis, [(i, i ^ 1) for i in range(size)])


def shards(prompts, target_embed, labels, lengths, attn_gain, w_qkv, w_out, final_gain, w_vocab):
    n_model = lax.axis_size("mp")
    n_seq = lax.axis_size("dp")
    my_seq = lax.axis_index("dp")
    prompts_here, prompt_len, model_width = prompts.shape
    seq_count, target_len, _ = target_embed.shape
    hops = range(1, n_model)
    paired = n_seq % 2 == 0
    stride = 2 if paired else 1
    unit = seq_count * target_len

    flat_labels = labels.reshape(-1)
    pair_labels = swap_pair(flat_labels, "dp") if paired else None
    got_out = []
    for k in hops:
        got_out.append(shift_by(peer_piece(w_out, "prompt"), "mp", k))
    flat_embed = target_embed.reshape(-1, model_width)
    if paired:
        got_embed = swap_pair(peer_piece(flat_embed, "prompt"), "dp")
    parts = 4 if w_vocab.shape[1] % 512 == 0 else 1
    part_cols = w_vocab.shape[1] // parts
    vocab_jobs = [(k, c) for k in range(stride, n_seq, stride) for c in range(parts)]
    own_piece = peer_piece(w_vocab, "prompt")

    def fetch(n):
        k, c = vocab_jobs[n]
        return shift_by(own_piece[:, c * part_cols : (c + 1) * part_cols], "dp", k)

    got_vocab = [fetch(0)]

    pad_len = -(-prompt_len // 128) * 128
    positions = jnp.concatenate(
        [prompt_len + jnp.arange(target_len, dtype=jnp.int32)] * seq_count
        + [jnp.arange(pad_len, dtype=jnp.int32)] * prompts_here
    )
    cosine, sine = rope_tables(positions)
    qkv = project(flat_embed, prompts, pad_len, attn_gain, w_qkv, cosine, sine)
    ctx = attend(qkv, prompts_here, target_len, seq_count, prompt_len, pad_len)
    ctx = ctx.reshape(prompts_here * unit, -1)

    if paired:
        ctx_pair = swap_pair(ctx, "dp")
    other_a = jnp.concatenate([shift_by(ctx, "mp", k) for k in hops], axis=1)
    for n in range(1, len(vocab_jobs)):
        got_vocab.append(fetch(n))

    out_pieces, out_offsets = [], []
    for n, got in enumerate(got_out):
        held = spread(got, "prompt")
        if got.shape[0] % LANES:
            held = [(assemble(held), jnp.int32(0))]
        for piece, owner in held:
            out_pieces.append(piece)
            out_offsets.append(n * w_out.shape[0] + owner * piece.shape[0])
    vocab_sets = []
    for n, got in enumerate(got_vocab):
        held = spread(got, "prompt")
        first = (ring_source("dp", vocab_jobs[n][0]) * n_model + lax.axis_index("mp")) * w_vocab.shape[1]
        first = first + vocab_jobs[n][1] * part_cols
        scalars = jnp.stack([first] + [o * p.shape[0] for p, o in held]).astype(jnp.int32)
        vocab_sets.append(([p for p, _ in held], scalars))

    def tiled(flat):
        return jnp.tile(flat, (prompts_here,) + (1,) * (flat.ndim - 1))

    def numbers(values):
        return jnp.stack([jnp.asarray(v, jnp.int32) for v in values])

    own_first = (my_seq * n_model + lax.axis_index("mp")) * w_vocab.shape[1]
    count = 2 if paired else 1
    ids = [tiled(flat_labels)]
    got = score_own(
        0, count, [], ctx, other_a, final_gain, ids[0], w_out, w_vocab, out_pieces, [flat_embed],
        numbers([own_first] + out_offsets + [0]),
    )
    if paired:
        other_b = jnp.concatenate([shift_by(ctx_pair, "mp", k) for k in hops], axis=1)
        held = spread(got_embed, "prompt")
        height = got_embed.shape[0]
        if height % LANES:
            held = [(assemble(held), 0)]
        ids.append(tiled(pair_labels))
        got = score_own(
            1, count, list(got), ctx_pair, other_b, final_gain, ids[1], w_out, w_vocab, out_pieces,
            [p for p, _ in held],
            numbers([own_first] + out_offsets + [o * height for _, o in held]),
        )
    rows, scale, *stats = [v.reshape((-1,) + v.shape[2:]) for v in got]
    every_id = jnp.concatenate(ids)
    for pieces, scalars in vocab_sets:
        stats = score_far(rows, scale, every_id, stats, pieces, scalars)

    folded = fold_lanes(stats)
    half = folded.shape[1] // count
    merged = folded[:, :half]
    if paired:
        merged = combine_stats(merged, swap_pair(folded[:, half:], "dp"))
    for other in [shift_by(merged, "mp", k) for k in hops]:
        merged = combine_stats(merged, other)
    losses = merged[0] + jnp.log(merged[1]) - merged[2]
    losses = losses.reshape(prompts_here, seq_count, target_len)
    valid = jnp.arange(target_len, dtype=jnp.int32)[None, :] < lengths[:, None]
    token_loss = jnp.where(valid[None], losses, 0.0)
    prompt_sums = jnp.sum(token_loss, axis=(1, 2))
    counted = jnp.sum(lengths).astype(jnp.float32)
    sums = jnp.sum(small_gather(jnp.concatenate([prompt_sums, counted[None]]), "dp"), axis=0)
    table = small_gather(sums, "prompt")
    prompt_loss = table[:, :prompts_here].reshape(-1) / table[0, prompts_here]
    return (token_loss, prompt_loss)


def solution(mesh):
    return jax.shard_map(
        shards,
        mesh=mesh,
        in_specs=(
            P("prompt", None, None),
            P("dp", None, None),
            P("dp", None),
            P("dp"),
            P(),
            P(None, None, "mp"),
            P("mp", None),
            P(),
            P(None, ("dp", "mp")),
        ),
        out_specs=(P("prompt", "dp", None), P()),
        check_vma=False,
    )
```
